32 devices in a mesh: dp: 4 (over x, core), graph: 8 (over z, y).
Axes of the slice: x: 2, y: 2, z: 4, core: 2. Of those that a mesh axis runs over, the one named last changes fastest.
Arguments:
- node_feats: bfloat16 [4, 128, 3712], P('dp', 'graph'), may hold values from -6 to 6
- node_cotan: bfloat16 [4, 128, 3712], P('dp', 'graph'), may hold values from -6 to 6
- source: int32 [4, 2560], P('dp', 'graph'), may hold values from 0 to 127, as said below
- target: int32 [4, 2560], P('dp', 'graph'), may hold values from 0 to 127, as said below
- angle: float32 [4, 2560], P('dp', 'graph'), may hold values from -3.140625 to 3.140625
- w_zero: bfloat16 [896, 896], replicated, may hold values from -0.1875 to 0.1875
- w_one: bfloat16 [768, 1536], replicated, may hold values from -0.21875 to 0.21875
- w_two: bfloat16 [640, 1280], replicated, may hold values from -0.25 to 0.25
Outputs:
- grad_nodes: bfloat16 [4, 128, 3712], P('dp', 'graph')
- grad_zero: float32 [896, 896], P('graph')
- grad_one: float32 [768, 1536], P('graph')
- grad_two: float32 [640, 1280], P('graph')
The draws below stay inside these ranges and needn't reach their ends.
Inputs may be any that keep to these rules, and one draw needn't show every extreme that they name: `source`: the edges at positions d * 320 to (d + 1) * 320 - 1 of a batch have both ends among atoms d * 16 - 8 to (d + 1) * 16 + 7; the first and the last of these atoms that lie in the batch are named on every device; no edge joins an atom to itself. `target`: as for source, with the same ranges per device.
All inputs are finite; a program needn't handle non-finite values.
Results may differ from the reference program's by a relative error of at most 0.0015.
The reference program's roundings to bfloat16 on the way count: a program that leaves them out, or rounds other values in their place, can miss the bound.
Values may be sent and summed in bfloat16 or wider, within the bound.
No kernel may reach another device: no remote copies, remote signals or barrier semaphores. Data moves between devices by JAX's collectives and lax.ppermute only.
A program may use at most 128 MiB of HBM per device.

```python
import jax
import jax.numpy as jnp
from jax import lax

C = 128
HEADS = 8
ATOM_DEV = 16
EDGE_DEV = 320
REACH = 8
ATOMS = 128
EDGES = 2560
GROUPS = 4


def edge_pair(key):
    folded = jax.random.fold_in(key, 4242)
    first_key, second_key = jax.random.split(folded)
    position = jnp.arange(EDGES, dtype=jnp.int32)
    device = position // EDGE_DEV
    within = position % EDGE_DEV
    lower = jnp.maximum(device * ATOM_DEV - REACH, 0)
    upper = jnp.minimum((device + 1) * ATOM_DEV + REACH, ATOMS)
    extent = upper - lower
    target = lower + jax.random.randint(first_key, (GROUPS, EDGES), 0, 1 << 24, dtype=jnp.int32) % extent
    offset = jax.random.randint(second_key, (GROUPS, EDGES), 0, 1 << 24, dtype=jnp.int32) % (extent - 1)
    source = lower + offset
    source = jnp.where(source >= target, source + 1, source)
    source = jnp.where(within == 0, lower, source)
    target = jnp.where(within == 0, upper - 1, target)
    source = jnp.where(within == 1, upper - 1, source)
    target = jnp.where(within == 1, lower, target)
    return (source.astype(jnp.int32), target.astype(jnp.int32))


def draw_source(key, part):
    return edge_pair(key)[0]


def draw_target(key, part):
    return edge_pair(key)[1]


def block_levels(rng, shape, shards, low, largest):
    factor_of = 1.0
    for axis_at, parts in shards:
        heights = jax.random.uniform(jax.random.fold_in(jax.random.fold_in(rng, 6), axis_at), (parts,), jnp.float32, low / len(shards), largest / len(shards))
        factor_of = factor_of * jnp.repeat(jnp.exp(heights), shape[axis_at] // parts).reshape((-1,) + (1,) * (len(shape) - 1 - axis_at))
    return factor_of


def centred(stream_key, shape, scale, limit, shards=(), kind=jnp.bfloat16):
    factor_of = block_levels(stream_key, shape, shards, -0.22, 0.18) if shards else 1.0
    values = jax.random.normal(stream_key, shape, jnp.float32) * scale * factor_of
    return jnp.minimum(jnp.maximum(values, -limit), limit).astype(kind)


def setup_inputs(seed: int = 0) -> dict:
    key_of = jax.random.split(jax.random.key(seed), 9)
    return {
        "node_feats": centred(key_of[0], (GROUPS, ATOMS, 29 * C), 1.0, 6.0, ((0, 4), (1, 8))),
        "node_cotan": centred(key_of[1], (GROUPS, ATOMS, 29 * C), 1.0, 6.0, ((0, 4), (1, 8))),
        "source": draw_source(jax.random.fold_in(key_of[8], 71), 0),
        "target": draw_target(jax.random.fold_in(key_of[8], 71), 0),
        "angle": jnp.clip(jax.random.uniform(key_of[4], (GROUPS, EDGES), jnp.float32, -3.140625, 3.140625), -3.140625, 3.140625),
        "w_zero": centred(key_of[5], (7 * C, 7 * C), (7 * C) ** -0.5, 0.1875),
        "w_one": centred(key_of[6], (6 * C, 12 * C), (6 * C) ** -0.5, 0.21875),
        "w_two": centred(key_of[7], (5 * C, 10 * C), (5 * C) ** -0.5, 0.25),
    }


def contract_rows(first, second):
    return lax.dot_general(first, second, (((0,), (0,)), ((), ())), preferred_element_type=jnp.float32)

def contract_cols(first, weight):
    return lax.dot_general(first, weight, (((1,), (1,)), ((), ())), preferred_element_type=jnp.float32)

def rotate(first, second, cosine, sine):
    return (cosine * first - sine * second, sine * first + cosine * second)

def per_head(block, channels, heads):
    count = block.shape[0]
    return block.reshape(count, -1, heads, channels // heads)

def edge_terms(feats, cotan, phases, w_zero, w_one, w_two, channels, heads):
    count = feats.shape[0]
    bounds = [0, 7 * channels, 13 * channels, 19 * channels, 24 * channels, 29 * channels]
    cos_one = jnp.cos(phases)[:, None]
    sin_one = jnp.sin(phases)[:, None]
    cos_two = jnp.cos(2.0 * phases)[:, None]
    sin_two = jnp.sin(2.0 * phases)[:, None]
    zero_in = feats[:, :bounds[1]]
    pieces = [feats[:, bounds[k]:bounds[k + 1]].astype(jnp.float32) for k in range(1, 5)]
    rot_p1, rot_n1 = rotate(pieces[0], pieces[1], cos_one, sin_one)
    rot_p2, rot_n2 = rotate(pieces[2], pieces[3], cos_two, sin_two)
    stack_one = jnp.concatenate([rot_p1.astype(jnp.bfloat16), rot_n1.astype(jnp.bfloat16)], 0)
    stack_two = jnp.concatenate([rot_p2.astype(jnp.bfloat16), rot_n2.astype(jnp.bfloat16)], 0)
    zero_out = jnp.dot(zero_in, w_zero, preferred_element_type=jnp.float32)
    prod_one = jnp.dot(stack_one, w_one, preferred_element_type=jnp.float32)
    prod_two = jnp.dot(stack_two, w_two, preferred_element_type=jnp.float32)
    half_one = 6 * channels
    half_two = 5 * channels
    out_p1 = prod_one[:count, :half_one] - prod_one[count:, half_one:]
    out_n1 = prod_one[:count, half_one:] + prod_one[count:, :half_one]
    out_p2 = prod_two[:count, :half_two] - prod_two[count:, half_two:]
    out_n2 = prod_two[:count, half_two:] + prod_two[count:, :half_two]
    scale = 1.0 / jnp.sqrt(jnp.float32(channels // heads))
    logits = per_head(zero_out[:, :channels], channels, heads).sum(axis=(1, 3)) * scale
    gate = jax.nn.sigmoid(logits)
    grads_in = [cotan[:, bounds[k]:bounds[k + 1]].astype(jnp.float32) for k in range(5)]
    du_zero = grads_in[0]
    du_p1, du_n1 = rotate(grads_in[1], grads_in[2], cos_one, sin_one)
    du_p2, du_n2 = rotate(grads_in[3], grads_in[4], cos_two, sin_two)
    dgate = jnp.zeros((count, heads), jnp.float32)
    for upstream, forward in ((du_zero, zero_out), (du_p1, out_p1), (du_n1, out_n1), (du_p2, out_p2), (du_n2, out_n2)):
        dgate = dgate + per_head(upstream * forward, channels, heads).sum(axis=(1, 3))
    dlogit = dgate * gate * (1.0 - gate) * scale

    def gated(block):
        shaped = per_head(block, channels, heads) * gate[:, None, :, None]
        return shaped.reshape(count, -1)
    dz_zero = gated(du_zero)
    dz_zero = jnp.concatenate([dz_zero[:, :channels] + jnp.repeat(dlogit, channels // heads, axis=1), dz_zero[:, channels:]], 1)
    dz_zero = dz_zero.astype(jnp.bfloat16)
    dz_p1, dz_n1, dz_p2, dz_n2 = (gated(du_p1), gated(du_n1), gated(du_p2), gated(du_n2))
    grad_one = jnp.concatenate([jnp.concatenate([dz_p1, dz_n1], 1), jnp.concatenate([dz_n1, -dz_p1], 1)], 0).astype(jnp.bfloat16)
    grad_two = jnp.concatenate([jnp.concatenate([dz_p2, dz_n2], 1), jnp.concatenate([dz_n2, -dz_p2], 1)], 0).astype(jnp.bfloat16)
    back_zero = contract_cols(dz_zero, w_zero)
    back_one = contract_cols(grad_one, w_one)
    back_two = contract_cols(grad_two, w_two)
    dp_one, dn_one = rotate(back_one[:count], back_one[count:], cos_one, -sin_one)
    dp_two, dn_two = rotate(back_two[:count], back_two[count:], cos_two, -sin_two)
    node_terms = jnp.concatenate([back_zero, dp_one, dn_one, dp_two, dn_two], 1)
    return (node_terms, contract_rows(zero_in, dz_zero), contract_rows(stack_one, grad_one), contract_rows(stack_two, grad_two))

def reference(node_feats, node_cotan, source, target, angle, w_zero, w_one, w_two):
    channels = w_zero.shape[0] // 7
    blocks = EDGES // EDGE_DEV
    width = node_feats.shape[2]

    def one_group(items):
        feats, cotan, sources, targets, phases = items

        def advance(carry, block):
            grads, acc_zero, acc_one, acc_two = carry
            src_rows, dst_rows, block_phases = block
            node_terms, part_zero, part_one, part_two = edge_terms(feats[src_rows], cotan[dst_rows], block_phases, w_zero, w_one, w_two, channels, HEADS)
            return ((grads.at[src_rows].add(node_terms), acc_zero + part_zero, acc_one + part_one, acc_two + part_two), None)
        start = (jnp.zeros((ATOMS, width), jnp.float32), jnp.zeros(w_zero.shape, jnp.float32), jnp.zeros(w_one.shape, jnp.float32), jnp.zeros(w_two.shape, jnp.float32))
        blocked = (sources.reshape(blocks, EDGE_DEV).astype(jnp.int32), targets.reshape(blocks, EDGE_DEV).astype(jnp.int32), phases.reshape(blocks, EDGE_DEV))
        (grads, acc_zero, acc_one, acc_two), _ = lax.scan(advance, start, blocked)
        return (grads.astype(jnp.bfloat16), acc_zero, acc_one, acc_two)
    grads, acc_zero, acc_one, acc_two = lax.map(one_group, (node_feats, node_cotan, source, target, angle))
    return (grads, acc_zero.sum(0) / GROUPS, acc_one.sum(0) / GROUPS, acc_two.sum(0) / GROUPS)
```

```python
import jax
import jax.numpy as jnp
from jax import lax
from jax.experimental import pallas as pl
from jax.experimental.pallas import tpu as pltpu
from jax.sharding import PartitionSpec as P

HEADS = 8
LEVELS = 7
ROWS = 16
LANES = 128
F32 = jnp.float32
BF16 = jnp.bfloat16


def mm(first, second):
    return lax.dot_general(first, second, (((1,), (0,)), ((), ())), preferred_element_type=F32)


def mm_t(first, second):
    return lax.dot_general(first, second, (((1,), (1,)), ((), ())), preferred_element_type=F32)


def pieces(value, count):
    out = []
    rest = value
    for _ in range(count):
        part = rest.astype(BF16)
        out.append(part)
        rest = rest - part.astype(F32)
    return out


def one_hot(index, shape, dim):
    return jnp.where(lax.broadcasted_iota(jnp.int32, shape, dim) == index, 1.0, 0.0).astype(F32)


def chunks(width, step=256):
    return [(lo, min(lo + step, width)) for lo in range(0, width, step)]


def head_mask(channels, heads):
    size = channels // heads
    row = lax.broadcasted_iota(jnp.int32, (channels, channels), 0) // size
    col = lax.broadcasted_iota(jnp.int32, (channels, channels), 1) // size
    return jnp.where(row == col, 1.0, 0.0).astype(BF16)


def head_sum(value, channels, heads):
    mask = head_mask(channels, heads)
    total = None
    for part in pieces(value, 3):
        term = mm(part, mask)
        total = term if total is None else total + term
    return total


class Tiles:
    def __init__(self, rows, cols, graph, parts):
        self.rows = rows // graph
        self.cols = cols
        self.graph = graph
        self.down = -(-self.rows // ROWS)
        self.across = cols // LANES
        self.count = self.down * self.across
        self.parts = parts
        self.each = -(-self.count // parts)
        self.shape = (parts, graph, self.each + 1, ROWS, LANES)

    def store(self, ref, block, lo):
        for g in range(self.graph):
            for i in range(self.down):
                r0 = i * ROWS
                r1 = min(r0 + ROWS, self.rows)
                for j in range(block.shape[1] // LANES):
                    tile = i * self.across + lo // LANES + j
                    ref[tile // self.each, g, tile % self.each, : r1 - r0, :] = block[
                        g * self.rows + r0 : g * self.rows + r1, j * LANES : (j + 1) * LANES
                    ]

    def finish(self, ref, exponent):
        level = jnp.broadcast_to(exponent, (ROWS, LANES))
        for q in range(self.parts):
            for g in range(self.graph):
                ref[q, g, self.each] = level
        for tile in range(self.count, self.parts * self.each):
            for g in range(self.graph):
                ref[tile // self.each, g, tile % self.each] = jnp.zeros((ROWS, LANES), F32)

    def rebuild(self, tiles):
        flat = tiles.reshape(self.parts * self.each, ROWS, LANES)[: self.count]
        grid = flat.reshape(self.down, self.across, ROWS, LANES).transpose(0, 2, 1, 3)
        return grid.reshape(self.down * ROWS, self.cols)[: self.rows]


def level_of(bound):
    return jnp.floor(jnp.log2(jnp.maximum(bound, 1e-30))) + 2.0


def top(value):
    return jnp.max(jnp.max(jnp.abs(value), axis=1, keepdims=True), axis=0, keepdims=True)


def wgrad_pair(tiles, ref, xst, dref, width, count):
    turned = xst.T
    for lo, hi in chunks(2 * width):
        if hi <= width:
            upper = dref[:, lo:hi]
            lower = dref[:, width + lo : width + hi]
        elif lo >= width:
            upper = dref[:, lo:hi]
            lower = -dref[:, lo - width : hi - width]
        else:
            upper = dref[:, lo:hi]
            lower = jnp.concatenate([dref[:, width + lo :], -dref[:, : hi - width]], 1)
        tiles.store(ref, mm(turned, jnp.concatenate([upper, lower], 0)), lo)


def make_first(channels, heads, tiles):
    z, w1, w2 = LEVELS * channels, (LEVELS - 1) * channels, (LEVELS - 2) * channels
    b1, b2 = z + 2 * w1, z + 2 * w1 + 2 * w2

    def body(table, src, dst, trig, wz, x1, d1, x2, d2, gate_out, cot_out, level_out, grad):
        count = src.shape[0]
        atoms = table.shape[1]
        pick = one_hot(src[...], (count, atoms), 1).astype(BF16)
        aim = one_hot(dst[...], (count, atoms), 1).astype(BF16)
        feat = table.at[0]
        cot = table.at[1]
        scale = 1.0 / (channels // heads) ** 0.5
        logits = mm(feat[:, :z], wz[...])
        gate_node = jax.nn.sigmoid(head_sum(logits, channels, heads) * scale)
        gate = sum(mm(pick, part) for part in pieces(gate_node, 3))
        gate_out[...] = gate
        cot_out[...] = mm(aim, cot[...]).astype(BF16)

        def turn(lo, width, cosine, sine, x, d):
            for j in range(width // channels):
                at = slice(lo + j * channels, lo + (j + 1) * channels)
                bt = slice(lo + width + j * channels, lo + width + (j + 1) * channels)
                p = mm(pick, feat[:, at])
                n = mm(pick, feat[:, bt])
                to = slice(j * channels, (j + 1) * channels)
                x[:count, to] = (cosine * p - sine * n).astype(BF16)
                x[count:, to] = (sine * p + cosine * n).astype(BF16)
                p = cot_out[:, at].astype(F32)
                n = cot_out[:, bt].astype(F32)
                d[:, to] = (gate * (cosine * p - sine * n)).astype(BF16)
                d[:, width + j * channels : width + (j + 1) * channels] = (
                    gate * (sine * p + cosine * n)
                ).astype(BF16)

        turn(z, w1, trig[:, 0:1], trig[:, 1:2], x1, d1)
        turn(b1, w2, trig[:, 2:3], trig[:, 3:4], x2, d2)
        wgrad_pair(tiles, grad, x1[...], d1, w1, count)
        bound = top(feat[...].astype(F32)) * top(cot[...].astype(F32)) * (4.1 * count)
        level = level_of(bound)
        level_out[...] = jnp.broadcast_to(level, level_out.shape)
        tiles.finish(grad, level)

    return body


def make_second(channels, tiles):
    w2 = (LEVELS - 2) * channels

    def body(x2, d2, level_in, grad):
        wgrad_pair(tiles, grad, x2[...], d2, w2, d2.shape[0])
        tiles.finish(grad, level_in[0:1, 0:1])

    return body


def make_third(channels, heads, tiles):
    z, w1, w2 = LEVELS * channels, (LEVELS - 1) * channels, (LEVELS - 2) * channels
    b1 = z + 2 * w1

    def body(table, src, trig, src_row, trig_row, x1, d1, x2, d2, gate_in, cot, wz, wo, wt, grad, nodes):
        count = src.shape[0]
        atoms = table.shape[1]
        feat = table.at[0]
        gate = gate_in[...]
        pick = one_hot(src[...], (count, atoms), 1).astype(BF16)
        place = one_hot(src_row[...], (atoms, count), 0)
        scale = 1.0 / (channels // heads) ** 0.5

        dgate = jnp.zeros((count, channels), F32)
        node_zero = mm(feat[:, :z], wz[...])
        wide = jnp.concatenate(pieces(node_zero, 3), 0)
        pick_wide = jnp.concatenate([pick, pick, pick], 1)
        for lo, hi in chunks(z):
            out = mm(pick_wide, wide[:, lo:hi])
            term = cot[:, lo:hi].astype(F32) * out
            for k in range((hi - lo) // channels):
                dgate = dgate + term[:, k * channels : (k + 1) * channels]

        def forward(dgate, lo0, width, cosine, sine, x, w):
            rp = x[:count, :]
            rn = x[count:, :]
            for lo, hi in chunks(width):
                wa = w[:, lo:hi]
                wb = w[:, width + lo : width + hi]
                out_p = mm(rp, wa) - mm(rn, wb)
                out_n = mm(rp, wb) + mm(rn, wa)
                p = cot[:, lo0 + lo : lo0 + hi].astype(F32)
                n = cot[:, lo0 + width + lo : lo0 + width + hi].astype(F32)
                term = (cosine * p - sine * n) * out_p + (sine * p + cosine * n) * out_n
                for k in range((hi - lo) // channels):
                    dgate = dgate + term[:, k * channels : (k + 1) * channels]
            return dgate

        dgate = forward(dgate, z, w1, trig[:, 0:1], trig[:, 1:2], x1, wo)
        dgate = forward(dgate, b1, w2, trig[:, 2:3], trig[:, 3:4], x2, wt)
        dlogit = head_sum(dgate, channels, heads) * gate * (1.0 - gate) * scale
        dz = []
        for j in range(LEVELS):
            block = gate * cot[:, j * channels : (j + 1) * channels].astype(F32)
            if j == 0:
                block = block + dlogit
            dz.append(block.astype(BF16))
        dz = jnp.concatenate(dz, 1)

        node_dz = mm(place.astype(BF16), dz)
        parts = pieces(node_dz, 3)
        turned = feat[:, :z].astype(F32).T.astype(BF16)
        turned = jnp.concatenate([turned, turned, turned], 1)
        stack = jnp.concatenate(parts, 0)
        for lo, hi in chunks(z):
            tiles.store(grad, mm(turned, stack[:, lo:hi]), lo)
        bound = top(feat[:, :z].astype(F32)) * top(dz.astype(F32)) * (1.01 * count)
        tiles.finish(grad, level_of(bound))

        back = mm_t(stack, wz[...])
        nodes[:, :z] = back[:atoms] + back[atoms : 2 * atoms] + back[2 * atoms :]

        def backward(lo0, width, cosine, sine, d, w):
            terms = pieces(place * cosine, 2) + pieces(place * sine, 2)
            spread = mm(jnp.concatenate(terms, 0), d[...])
            by_c = spread[:atoms] + spread[atoms : 2 * atoms]
            by_s = spread[2 * atoms : 3 * atoms] + spread[3 * atoms :]
            t1 = by_c[:, :width] + by_s[:, width:]
            t2 = by_c[:, width:] - by_s[:, :width]
            plus = pieces(jnp.concatenate([t1, t2], 1), 2)
            minus = pieces(jnp.concatenate([t2, -t1], 1), 2)
            back = mm_t(jnp.concatenate(plus + minus, 0), w[...])
            nodes[:, lo0 : lo0 + width] = back[:atoms] + back[atoms : 2 * atoms]
            nodes[:, lo0 + width : lo0 + 2 * width] = (
                back[2 * atoms : 3 * atoms] + back[3 * atoms :]
            )

        backward(z, w1, trig_row[0:1, :], trig_row[1:2, :], d1, wo)
        backward(b1, w2, trig_row[2:3, :], trig_row[3:4, :], d2, wt)

    return body


def bits_of(size):
    return [k for k in range(size.bit_length() - 1)]


def main_mask(ndim, each):
    shape = [1] * ndim
    shape[-3] = each + 1
    return lax.broadcasted_iota(jnp.int32, tuple(shape), ndim - 3) < each


def level_in(value):
    for _ in range(value.ndim - 3):
        value = value[0]
    return value[-1, 0, 0]


def encode(value, each):
    level = level_in(value)
    factor = jnp.where(main_mask(value.ndim, each), jnp.exp2(15.0 - level), 1.0)
    return (value * factor).astype(jnp.float16)


def decode(message, each):
    value = message.astype(F32)
    factor = jnp.where(main_mask(value.ndim, each), jnp.exp2(level_in(value) - 15.0), 1.0)
    return value * factor


def combine(first, second, each):
    both = jnp.where(
        main_mask(first.ndim, each), first + second, jnp.maximum(first, second) + 1.0
    )
    return both


def exchange(parts, bit, me):
    size = lax.axis_size("dp")
    mine = (me >> bit) & 1
    sends = [
        encode(lax.dynamic_index_in_dim(value, 1 - mine, 0, False), tiles.each)
        for value, tiles in parts
    ]
    return mine, sends, [(i, i ^ (1 << bit)) for i in range(size)]


def halve(parts, bit, me):
    mine, sends, route = exchange(parts, bit, me)
    got = join(sends)
    got = lax.ppermute(got, "dp", route)
    out = []
    for (value, tiles), message in zip(parts, split(got, parts)):
        keep = lax.dynamic_index_in_dim(value, mine, 0, False)
        out.append((combine(keep, decode(message, tiles.each), tiles.each), tiles))
    return out


def join(values):
    return values[0] if len(values) == 1 else jnp.concatenate(values, axis=values[0].ndim - 3)


def split(value, parts):
    out = []
    at = 0
    for _, tiles in parts:
        out.append(lax.slice_in_dim(value, at, at + tiles.each + 1, axis=value.ndim - 3))
        at += tiles.each + 1
    return out


def over_graph(parts):
    sent = join([encode(value, tiles.each) for value, tiles in parts])
    got = lax.all_to_all(sent, "graph", 0, 0, tiled=True)
    out = []
    for (_, tiles), message in zip(parts, split(got, parts)):
        value = message.astype(F32)
        factor = jnp.exp2(value[:, -1:, :1, :1] - 15.0)
        out.append(((value[:, : tiles.each] * factor).sum(0), tiles))
    return out


def regather(parts, me):
    size = lax.axis_size("dp")
    whole = join([value for value, _ in parts])[None]
    for bit in reversed(bits_of(size)):
        other = lax.ppermute(whole, "dp", [(i, i ^ (1 << bit)) for i in range(size)])
        low = ((me >> bit) & 1) == 0
        whole = jnp.concatenate([jnp.where(low, whole, other), jnp.where(low, other, whole)], 0)
    out = []
    at = 0
    for _, tiles in parts:
        out.append(tiles.rebuild(whole[:, at : at + tiles.each]) / size)
        at += tiles.each
    return out


def call(body, outs, flops, *args):
    return pl.pallas_call(
        body,
        out_shape=outs,
        in_specs=[pl.BlockSpec(memory_space=pltpu.VMEM)] * len(args),
        out_specs=jax.tree.map(lambda _: pl.BlockSpec(memory_space=pltpu.VMEM), outs),
        compiler_params=pltpu.CompilerParams(vmem_limit_bytes=60 * 1024 * 1024),
        cost_estimate=pl.CostEstimate(flops=flops, bytes_accessed=1 << 24, transcendentals=0),
    )(*args)


def shards(node_feats, node_cotan, source, target, angle, w_zero, w_one, w_two):
    atom_count = node_feats.shape[1]
    row_width = node_feats.shape[2]
    channels = row_width // 29
    edges = source.shape[1]
    graph = lax.axis_size("graph")
    size = lax.axis_size("dp")
    position = lax.axis_index("graph")
    me = lax.axis_index("dp")
    reach = atom_count // 2
    w1, w2 = (LEVELS - 1) * channels, (LEVELS - 2) * channels

    up = [(i, i + 1) for i in range(graph - 1)]
    down = [(i + 1, i) for i in range(graph - 1)]
    own = jnp.stack([node_feats[0], node_cotan[0]], 0)
    before = lax.ppermute(own[:, atom_count - reach :], "graph", up)
    after = lax.ppermute(own[:, :reach], "graph", down)
    table = jnp.concatenate([before, own, after], 1)
    first_atom = position * atom_count - reach
    src = source[0] - first_atom
    dst = target[0] - first_atom
    phases = angle[0]
    trig_row = jnp.stack(
        [jnp.cos(phases), jnp.sin(phases), jnp.cos(2.0 * phases), jnp.sin(2.0 * phases)], 0
    )
    trig = trig_row.T

    t_one = Tiles(*w_one.shape, graph, size)
    t_two = Tiles(*w_two.shape, graph, size)
    t_zero = Tiles(*w_zero.shape, graph, size)
    shape = jax.ShapeDtypeStruct
    x1, d1, x2, d2, gate, cot, level, grad_one = call(
        make_first(channels, HEADS, t_one),
        (
            shape((2 * edges, w1), BF16),
            shape((edges, 2 * w1), BF16),
            shape((2 * edges, w2), BF16),
            shape((edges, 2 * w2), BF16),
            shape((edges, channels), F32),
            shape((edges, row_width), BF16),
            shape((8, LANES), F32),
            shape(t_one.shape, F32),
        ),
        3_000_000_000,
        table,
        src[:, None],
        dst[:, None],
        trig,
        w_zero[:, :channels],
    )
    grad_two = call(
        make_second(channels, t_two), shape(t_two.shape, F32), 1_200_000_000, x2, d2, level
    )
    grad_zero, nodes = call(
        make_third(channels, HEADS, t_zero),
        (shape(t_zero.shape, F32), shape((atom_count + 2 * reach, row_width), F32)),
        4_000_000_000,
        table,
        src[:, None],
        trig,
        src[None, :],
        trig_row,
        x1,
        d1,
        x2,
        d2,
        gate,
        cot,
        w_zero,
        w_one,
        w_two,
    )

    from_next = lax.ppermute(nodes[:reach], "graph", down)
    from_prev = lax.ppermute(nodes[atom_count + reach :], "graph", up)
    rows = nodes[reach : reach + atom_count]
    rows = rows + jnp.concatenate([from_prev, from_next], 0)
    grad_nodes = rows.astype(BF16)[None]

    def paired(value):
        return value.reshape((2,) * len(bits_of(size)) + value.shape[1:])

    one = [(paired(grad_one), t_one)]
    rest = [(paired(grad_two), t_two), (paired(grad_zero), t_zero)]
    groups = [one, rest]
    for bit in bits_of(size):
        groups = [halve(parts, bit, me) for parts in groups]
    groups = [over_graph(parts) for parts in groups]
    (one,), (two, zero) = [regather(parts, me) for parts in groups]
    return (grad_nodes, zero, one, two)


def solution(mesh):
    return jax.shard_map(
        shards,
        mesh=mesh,
        in_specs=(
            P("dp", "graph", None),
            P("dp", "graph", None),
            P("dp", "graph"),
            P("dp", "graph"),
            P("dp", "graph"),
            P(),
            P(),
            P(),
        ),
        out_specs=(P("dp", "graph", None), P("graph", None), P("graph", None), P("graph", None)),
        check_vma=False,
    )
```

```python
import jax
import jax.numpy as jnp
from jax import lax
from jax.experimental import pallas as pl
from jax.experimental.pallas import tpu as pltpu
from jax.sharding import PartitionSpec as P


HEADS = 8
LEVELS = 7
ROWS = 16
LANES = 128
F32 = jnp.float32
BF16 = jnp.bfloat16
F16 = jnp.float16


def mm(first, second):
    return lax.dot_general(first, second, (((1,), (0,)), ((), ())), preferred_element_type=F32)


def mm_t(first, second):
    return lax.dot_general(first, second, (((1,), (1,)), ((), ())), preferred_element_type=F32)


def pieces(value, count):
    out = []
    rest = value
    for _ in range(count):
        part = rest.astype(BF16)
        out.append(part)
        rest = rest - part.astype(F32)
    return out


def one_hot(index, shape, dim):
    count = lax.broadcasted_iota(jnp.int32, shape, dim).astype(F32)
    return jnp.where(count == index, 1.0, 0.0).astype(F32)


def chunks(width, step=256):
    return [(lo, min(lo + step, width)) for lo in range(0, width, step)]


def head_mask(channels, heads):
    size = channels // heads
    row = lax.broadcasted_iota(jnp.int32, (channels, channels), 0) // size
    col = lax.broadcasted_iota(jnp.int32, (channels, channels), 1) // size
    return jnp.where(row == col, 1.0, 0.0).astype(BF16)


def head_sum(value, channels, heads):
    mask = head_mask(channels, heads)
    total = None
    for part in pieces(value, 3):
        term = mm(part, mask)
        total = term if total is None else total + term
    return total


class Tiles:
    def __init__(self, rows, cols, graph, parts, spare=0):
        self.rows = rows // graph
        self.cols = cols
        self.graph = graph
        self.down = -(-self.rows // ROWS)
        self.across = cols // LANES
        self.count = self.down * self.across
        self.parts = parts
        self.each = -(-self.count // parts) + spare
        self.block = (graph, self.each + 1, ROWS, LANES)

    def scratch(self):
        return pltpu.VMEM((2, self.parts // 2) + self.block, F32)

    def store(self, ref, flip, block, lo):
        half = self.parts // 2
        for g in range(self.graph):
            for i in range(self.down):
                r0 = i * ROWS
                r1 = min(r0 + ROWS, self.rows)
                for j in range(block.shape[1] // LANES):
                    tile = i * self.across + lo // LANES + j
                    q = tile // self.each
                    ref[flip ^ (q // half), q % half, g, tile % self.each, : r1 - r0, :] = block[
                        g * self.rows + r0 : g * self.rows + r1, j * LANES : (j + 1) * LANES
                    ]

    def blank(self, ref, flip):
        half = self.parts // 2
        for tile in range(self.count, self.parts * self.each):
            q = tile // self.each
            for g in range(self.graph):
                ref[flip ^ (q // half), q % half, g, tile % self.each] = jnp.zeros(
                    (ROWS, LANES), F32
                )


def is_level(value):
    axis = value.ndim - 3
    return lax.broadcasted_iota(jnp.int32, value.shape, axis) == value.shape[axis] - 1


def unit_of(value, rows):
    tile = value[..., -1:, :rows, :].astype(F32)
    tile = tile * tile
    tile = tile * tile
    return jnp.broadcast_to(tile * tile, value.shape)


def encode(value, rows):
    return jnp.where(is_level(value), value, value * (32768.0 / unit_of(value, rows))).astype(F16)


def decode(message, rows):
    value = message.astype(F32)
    return jnp.where(is_level(value), value, value * (unit_of(message, rows) * (1.0 / 32768.0)))


def combine(first, second):
    return jnp.where(is_level(first), jnp.maximum(first, second), first + second)


def level_of(bound):
    level = jnp.full(bound.shape, 2.0**-12, F32)
    for k in range(-11, 9):
        level = jnp.where(bound > 2.0 ** (8 * (k - 1)), 2.0**k, level)
    return level


def top(value):
    return jnp.max(jnp.max(jnp.abs(value), axis=1, keepdims=True), axis=0, keepdims=True)


def wgrad_pair(tiles, ref, flip, xst, dref, width):
    turned = xst.T
    for lo, hi in chunks(2 * width):
        if hi <= width:
            upper = dref[:, lo:hi]
            lower = dref[:, width + lo : width + hi]
        elif lo >= width:
            upper = dref[:, lo:hi]
            lower = -dref[:, lo - width : hi - width]
        else:
            upper = dref[:, lo:hi]
            lower = jnp.concatenate([dref[:, width + lo :], -dref[:, : hi - width]], 1)
        tiles.store(ref, flip, mm(turned, jnp.concatenate([upper, lower], 0)), lo)
    tiles.blank(ref, flip)


def hand_out(tiles, full, level, keep, send):
    tail = jnp.broadcast_to(level, (ROWS, LANES))
    for k, out in enumerate((keep, send)):
        for q in range(tiles.parts // 2):

            def step(g, carry):
                out[q, g, : tiles.each] = full[k, q, g, : tiles.each]
                out[q, g, tiles.each] = tail
                return carry

            lax.fori_loop(0, tiles.graph, step, 0)


def make_first(channels, heads, tiles, size, marks):
    z, w1, w2 = LEVELS * channels, (LEVELS - 1) * channels, (LEVELS - 2) * channels
    b1 = z + 2 * w1

    def body(
        me, table, cols, wz,
        x1, d1, x2, d2, gate_out, cot_out, feat_zero, level_out, keep, send, *rest,
    ):
        flags, full = rest[:-1], rest[-1]
        for flag, (axis, bit) in zip(flags, marks):
            value = (me[0 if axis == "dp" else 1] >> bit) & 1
            flag[...] = jnp.full((ROWS, LANES), value, jnp.int32).astype(F32)
        count = cols.shape[0]
        atoms = table.shape[1]
        flip = me[0] & 1
        feat = table.at[0]
        cot = table.at[1]
        feat_zero[...] = feat[:, :z]
        pick = one_hot(cols[:, 4:5], (count, atoms), 1).astype(BF16)
        aim = one_hot(cols[:, 5:6], (count, atoms), 1).astype(BF16)
        scale = 1.0 / (channels // heads) ** 0.5
        logits = mm(feat[:, :z], wz[...])
        gate_node = jax.nn.sigmoid(head_sum(logits, channels, heads) * scale)
        gate = sum(mm(pick, part) for part in pieces(gate_node, 3))
        gate_out[...] = gate
        cot_out[...] = mm(aim, cot[...]).astype(BF16)

        def turn(lo, width, cosine, sine, x, d):
            for j in range(width // channels):
                at = slice(lo + j * channels, lo + (j + 1) * channels)
                bt = slice(lo + width + j * channels, lo + width + (j + 1) * channels)
                p = mm(pick, feat[:, at])
                n = mm(pick, feat[:, bt])
                to = slice(j * channels, (j + 1) * channels)
                x[:count, to] = (cosine * p - sine * n).astype(BF16)
                x[count:, to] = (sine * p + cosine * n).astype(BF16)
                p = cot_out[:, at].astype(F32)
                n = cot_out[:, bt].astype(F32)
                d[:, to] = (gate * (cosine * p - sine * n)).astype(BF16)
                d[:, width + j * channels : width + (j + 1) * channels] = (
                    gate * (sine * p + cosine * n)
                ).astype(BF16)

        turn(z, w1, cols[:, 0:1], cols[:, 1:2], x1, d1)
        turn(b1, w2, cols[:, 2:3], cols[:, 3:4], x2, d2)
        wgrad_pair(tiles, full, flip, x1[...], d1, w1)
        bound = top(feat[...].astype(F32)) * top(cot[...].astype(F32)) * (4.1 * count * size * tiles.graph)
        level = level_of(bound)
        level_out[...] = jnp.broadcast_to(level, level_out.shape)
        hand_out(tiles, full, level, keep, send)

    return body


def make_second(channels, tiles):
    w2 = (LEVELS - 2) * channels

    def body(me, x2, d2, level_in, keep, send, full):
        wgrad_pair(tiles, full, me[0] & 1, x2[...], d2, w2)
        hand_out(tiles, full, level_in[0:1, 0:1], keep, send)

    return body


def make_forward(channels, heads):
    z, w1, w2 = LEVELS * channels, (LEVELS - 1) * channels, (LEVELS - 2) * channels
    b1 = z + 2 * w1

    def body(
        feat, cols, rows, x1, x2, gate_in, cot, wz, wo, wt, sums
    ):
        count = cols.shape[0]
        atoms = feat.shape[0]
        gate = gate_in[...]
        pick = one_hot(cols[:, 4:5], (count, atoms), 1).astype(BF16)
        place = one_hot(rows[4:5, :], (atoms, count), 0)
        scale = 1.0 / (channels // heads) ** 0.5

        dgate = jnp.zeros((count, channels), F32)
        node_zero = mm(feat[:, :z], wz[...])
        wide = jnp.concatenate(pieces(node_zero, 3), 0)
        pick_wide = jnp.concatenate([pick, pick, pick], 1)
        for lo, hi in chunks(z):
            out = mm(pick_wide, wide[:, lo:hi])
            term = cot[:, lo:hi].astype(F32) * out
            for k in range((hi - lo) // channels):
                dgate = dgate + term[:, k * channels : (k + 1) * channels]

        def forward(dgate, lo0, width, cosine, sine, x, w):
            rp = x[:count, :]
            rn = x[count:, :]
            for lo, hi in chunks(width):
                wa = w[:, lo:hi]
                wb = w[:, width + lo : width + hi]
                out_p = mm(rp, wa) - mm(rn, wb)
                out_n = mm(rp, wb) + mm(rn, wa)
                p = cot[:, lo0 + lo : lo0 + hi].astype(F32)
                n = cot[:, lo0 + width + lo : lo0 + width + hi].astype(F32)
                term = (cosine * p - sine * n) * out_p + (sine * p + cosine * n) * out_n
                for k in range((hi - lo) // channels):
                    dgate = dgate + term[:, k * channels : (k + 1) * channels]
            return dgate

        dgate = forward(dgate, z, w1, cols[:, 0:1], cols[:, 1:2], x1, wo)
        dgate = forward(dgate, b1, w2, cols[:, 2:3], cols[:, 3:4], x2, wt)
        dlogit = head_sum(dgate, channels, heads) * gate * (1.0 - gate) * scale
        dz = []
        for j in range(LEVELS):
            block = gate * cot[:, j * channels : (j + 1) * channels].astype(F32)
            if j == 0:
                block = block + dlogit
            dz.append(block.astype(BF16))
        dz = jnp.concatenate(dz, 1)

        node_dz = mm(place.astype(BF16), dz)
        parts = pieces(node_dz, 3)
        sums[0] = feat[...]
        for k in range(3):
            sums[k + 1] = parts[k]

    return body


def make_backward(channels):
    z, w1, w2 = LEVELS * channels, (LEVELS - 1) * channels, (LEVELS - 2) * channels
    b1 = z + 2 * w1

    def body(sums, rows, d1, d2, wz, wo, wt, nodes):
        count = rows.shape[1]
        atoms = sums.shape[1]
        place = one_hot(rows[4:5, :], (atoms, count), 0)
        stack = jnp.concatenate([sums[k] for k in (1, 2, 3)], 0)
        back = mm_t(stack, wz[...])
        nodes[:, :z] = back[:atoms] + back[atoms : 2 * atoms] + back[2 * atoms :]

        def backward(lo0, width, cosine, sine, d, w):
            terms = pieces(place * cosine, 2) + pieces(place * sine, 2)
            spread = mm(jnp.concatenate(terms, 0), d[...])
            by_c = spread[:atoms] + spread[atoms : 2 * atoms]
            by_s = spread[2 * atoms : 3 * atoms] + spread[3 * atoms :]
            t1 = by_c[:, :width] + by_s[:, width:]
            t2 = by_c[:, width:] - by_s[:, :width]
            plus = pieces(jnp.concatenate([t1, t2], 1), 2)
            minus = pieces(jnp.concatenate([t2, -t1], 1), 2)
            back = mm_t(jnp.concatenate(plus + minus, 0), w[...])
            nodes[:, lo0 : lo0 + width] = back[:atoms] + back[atoms : 2 * atoms]
            nodes[:, lo0 + width : lo0 + 2 * width] = (
                back[2 * atoms : 3 * atoms] + back[3 * atoms :]
            )

        backward(z, w1, rows[0:1, :], rows[1:2, :], d1, wo)
        backward(b1, w2, rows[2:3, :], rows[3:4, :], d2, wt)

    return body


def slot_of(me, size):
    bits = size.bit_length() - 1
    return sum(((me >> k) & 1) << (bits - 1 - k) for k in range(bits))


def make_zero(tiles, size):
    def body(me, *refs):
        sums, out, full = refs[:size], refs[size], refs[size + 1]
        left = [ref[0].astype(F32).T.astype(BF16) for ref in sums]
        left = jnp.concatenate([part for part in left for _ in range(3)], 1)
        right = jnp.concatenate([ref[k] for ref in sums for k in (1, 2, 3)], 0)
        for lo, hi in chunks(tiles.cols):
            tiles.store(full, 0, mm(left, right[:, lo:hi]), lo)
        tiles.blank(full, 0)
        rows = size * sums[0].shape[1]
        high = jnp.concatenate([ref[1].astype(F32) for ref in sums], 0)
        feats = jnp.concatenate([ref[0].astype(F32) for ref in sums], 0)
        level = level_of(top(feats) * top(high) * (1.02 * rows * tiles.graph))
        slot = slot_of(me[0], size)
        half = size // 2

        def step(g, carry):
            out[g, : tiles.each] = full[slot // half, slot % half, g, : tiles.each]
            out[g, tiles.each] = jnp.broadcast_to(level, (ROWS, LANES))
            return carry

        lax.fori_loop(0, tiles.graph, step, 0)

    return body


def make_output(tiles, size):
    def body(me, *refs):
        parts, out, flat = refs[:size], refs[size], refs[size + 1]
        for mask in range(size):
            flat[slot_of(me[0] ^ mask, size)] = parts[mask][...] * (1.0 / size)
        for tile in range(tiles.count):
            i, j = tile // tiles.across, tile % tiles.across
            r0, r1 = i * ROWS, min((i + 1) * ROWS, tiles.rows)
            out[r0:r1, j * LANES : (j + 1) * LANES] = flat[
                tile // tiles.each, tile % tiles.each, : r1 - r0
            ]

    return body


def call(body, outs, flops, mib, *args, scratch=(), scalars=1):
    vmem = pl.BlockSpec(memory_space=pltpu.VMEM)
    smem = pl.BlockSpec(memory_space=pltpu.SMEM)
    return pl.pallas_call(
        body,
        out_shape=outs,
        in_specs=[smem] * scalars + [vmem] * (len(args) - scalars),
        out_specs=jax.tree.map(lambda _: vmem, outs),
        scratch_shapes=scratch,
        compiler_params=pltpu.CompilerParams(vmem_limit_bytes=(mib << 20) + sum(ref.get_array_aval().size * 4 for ref in scratch)),
        cost_estimate=pl.CostEstimate(flops=flops, bytes_accessed=1 << 22, transcendentals=0),
    )(*args)


def swap(value, bit, axis="dp"):
    size = lax.axis_size(axis)
    return lax.ppermute(value, axis, [(i, i ^ (1 << bit)) for i in range(size)])


def shards(node_feats, node_cotan, source, target, angle, w_zero, w_one, w_two):
    atom_count = node_feats.shape[1]
    row_width = node_feats.shape[2]
    channels = row_width // 29
    edges = source.shape[1]
    graph = lax.axis_size("graph")
    size = lax.axis_size("dp")
    bits = size.bit_length() - 1
    position = lax.axis_index("graph")
    me = jnp.stack([lax.axis_index("dp"), position])
    reach = atom_count // 2
    atoms = atom_count + 2 * reach
    z, w1, w2 = LEVELS * channels, (LEVELS - 1) * channels, (LEVELS - 2) * channels
    shape = jax.ShapeDtypeStruct

    up = [(i, i + 1) for i in range(graph - 1)]
    down = [(i + 1, i) for i in range(graph - 1)]
    feats, cots = node_feats[0], node_cotan[0]
    before = lax.ppermute(
        jnp.stack([feats[atom_count - reach :], cots[atom_count - reach :]], 0), "graph", up
    )
    after = lax.ppermute(jnp.stack([feats[:reach], cots[:reach]], 0), "graph", down)
    first_atom = position * atom_count - reach
    src = (source[0] - first_atom).astype(F32)
    dst = (target[0] - first_atom).astype(F32)
    phases = angle[0]
    twice = 2.0 * phases
    trig = [jnp.cos(phases), jnp.sin(phases), jnp.cos(twice), jnp.sin(twice)]
    rows = jnp.stack(trig + [src, dst, src, dst], 0)
    cols = rows.T
    table = jnp.concatenate([before, jnp.stack([feats, cots], 0), after], 1)

    t_one = Tiles(*w_one.shape, graph, size)
    t_two = Tiles(*w_two.shape, graph, size)
    t_zero = Tiles(*w_zero.shape, graph, size, spare=1)

    def halves(tiles, parts):
        return (shape((parts,) + tiles.block, F32), shape((parts,) + tiles.block, F32))

    marks = [("dp", k) for k in range(bits)]
    marks += [("graph", k) for k in reversed(range(graph.bit_length() - 1))]
    x1, d1, x2, d2, gate, cot, feat_zero, level, keep_one, send_one, *flags = call(
        make_first(channels, HEADS, t_one, size, marks),
        (
            shape((2 * edges, w1), BF16),
            shape((edges, 2 * w1), BF16),
            shape((2 * edges, w2), BF16),
            shape((edges, 2 * w2), BF16),
            shape((edges, channels), F32),
            shape((edges, row_width), BF16),
            shape((atoms, z), BF16),
            shape((8, LANES), F32),
        )
        + halves(t_one, size // 2)
        + tuple(shape((ROWS, LANES), F32) for _ in marks),
        3_000_000_000,
        14,
        me,
        table,
        cols,
        w_zero[:, :channels],
        scratch=(t_one.scratch(),),
    )

    flags = dict(zip(marks, flags))

    def halving(value, left, steps, rows=ROWS):
        left = list(left)
        value = value.reshape((2,) * len(left) + value.shape[-3:])
        for axis, bit in steps:
            high = flags[axis, bit] > 0.5
            at = left.index((axis, bit))
            left.pop(at)
            low_half = lax.index_in_dim(value, 0, at, False)
            high_half = lax.index_in_dim(value, 1, at, False)
            send = encode(jnp.where(high, low_half, high_half), rows)
            got = swap(send, bit, axis)
            value = combine(jnp.where(high, high_half, low_half), decode(got, rows))
        return value

    def spread(tiles, value):
        parts = {0: value[: tiles.each]}
        for bit in reversed(range(bits)):
            parts.update({m | (1 << bit): swap(v, bit) for m, v in list(parts.items())})
        return call(
            make_output(tiles, size),
            shape((tiles.rows, tiles.cols), F32),
            50_000_000,
            4,
            me,
            *[parts[m] for m in range(size)],
            scratch=(pltpu.VMEM((size, tiles.each, ROWS, LANES), F32),),
        )

    keep_two, send_two = call(
        make_second(channels, t_two),
        halves(t_two, size // 2),
        1_200_000_000,
        6,
        me,
        x2,
        d2,
        level,
        scratch=(t_two.scratch(),),
    )
    one = combine(keep_one, swap(send_one, 0))
    two = combine(keep_two, swap(send_two, 0))
    over_dp = marks[1:bits]
    over_graph = list(reversed(marks[bits:]))
    one = halving(one, marks[1:], over_graph[:-1] + over_dp + over_graph[-1:])
    two = halving(two, marks[1:], over_dp + over_graph, rows=1)

    sums = call(
        make_forward(channels, HEADS),
        shape((4, atoms, z), BF16),
        4_000_000_000,
        8,
        feat_zero,
        cols,
        rows,
        x1,
        x2,
        gate,
        cot,
        w_zero,
        w_one,
        w_two,
        scalars=0,
    )
    nodes = call(
        make_backward(channels),
        shape((atoms, row_width), F32),
        2_000_000_000,
        8,
        sums,
        rows,
        d1,
        d2,
        w_zero,
        w_one,
        w_two,
        scalars=0,
    )

    from_next = lax.ppermute(nodes[:reach], "graph", down)
    from_prev = lax.ppermute(nodes[atom_count + reach :], "graph", up)
    owned = nodes[reach : reach + atom_count]
    owned = owned + jnp.concatenate([from_prev, from_next], 0)
    grad_nodes = owned.astype(BF16)[None]

    parts = {0: sums}
    for bit in reversed(range(bits)):
        parts.update({m | (1 << bit): swap(v, bit) for m, v in list(parts.items())})
    zero = call(
        make_zero(t_zero, size),
        shape(t_zero.block, F32),
        1_000_000_000,
        8,
        me,
        *[parts[m] for m in range(size)],
        scratch=(t_zero.scratch(),),
    )
    zero = halving(zero, marks[bits:], over_graph[1::-1] + over_graph[2:])
    grad_one = spread(t_one, one)
    grad_two = spread(t_two, two)
    grad_zero = spread(t_zero, zero)
    return (grad_nodes, grad_zero, grad_one, grad_two)


def solution(mesh):
    return jax.shard_map(
        shards,
        mesh=mesh,
        in_specs=(
            P("dp", "graph", None),
            P("dp", "graph", None),
            P("dp", "graph"),
            P("dp", "graph"),
            P("dp", "graph"),
            P(),
            P(),
            P(),
        ),
        out_specs=(P("dp", "graph", None), P("graph", None), P("graph", None), P("graph", None)),
        check_vma=False,
    )
```

```python
import jax
import jax.numpy as jnp
from jax import lax
from jax.experimental import pallas as pl
from jax.experimental.pallas import tpu as pltpu
from jax.sharding import PartitionSpec as P


HEADS = 8
LEVELS = 7
ROWS = 16
LANES = 128
F32 = jnp.float32
BF16 = jnp.bfloat16
F16 = jnp.float16


def mm(first, second):
    return lax.dot_general(first, second, (((1,), (0,)), ((), ())), preferred_element_type=F32)


def mm_t(first, second):
    return lax.dot_general(first, second, (((1,), (1,)), ((), ())), preferred_element_type=F32)


def pieces(value, count):
    out = []
    rest = value
    for _ in range(count):
        part = rest.astype(BF16)
        out.append(part)
        rest = rest - part.astype(F32)
    return out


def one_hot(index, shape, dim):
    count = lax.broadcasted_iota(jnp.int32, shape, dim).astype(F32)
    return jnp.where(count == index, 1.0, 0.0).astype(F32)


def chunks(width, step=256):
    return [(lo, min(lo + step, width)) for lo in range(0, width, step)]


def head_mask(channels, heads):
    size = channels // heads
    row = lax.broadcasted_iota(jnp.int32, (channels, channels), 0) // size
    col = lax.broadcasted_iota(jnp.int32, (channels, channels), 1) // size
    return jnp.where(row == col, 1.0, 0.0).astype(BF16)


def head_sum(value, channels, heads):
    mask = head_mask(channels, heads)
    total = None
    for part in pieces(value, 3):
        term = mm(part, mask)
        total = term if total is None else total + term
    return total


class Tiles:
    def __init__(self, rows, cols, graph, parts, spare=0):
        self.rows = rows // graph
        self.cols = cols
        self.graph = graph
        self.down = -(-self.rows // ROWS)
        self.across = cols // LANES
        self.count = self.down * self.across
        self.parts = parts
        self.each = -(-self.count // parts) + spare
        self.block = (graph, self.each + 1, ROWS, LANES)

    def scratch(self):
        return pltpu.VMEM((2, self.parts // 2) + self.block, F32)

    def store(self, ref, flip, block, lo):
        half = self.parts // 2
        for g in range(self.graph):
            for i in range(self.down):
                r0 = i * ROWS
                r1 = min(r0 + ROWS, self.rows)
                for j in range(block.shape[1] // LANES):
                    tile = i * self.across + lo // LANES + j
                    q = tile // self.each
                    ref[flip ^ (q // half), q % half, g, tile % self.each, : r1 - r0, :] = block[
                        g * self.rows + r0 : g * self.rows + r1, j * LANES : (j + 1) * LANES
                    ]

    def blank(self, ref, flip):
        half = self.parts // 2
        for tile in range(self.count, self.parts * self.each):
            q = tile // self.each
            for g in range(self.graph):
                ref[flip ^ (q // half), q % half, g, tile % self.each] = jnp.zeros(
                    (ROWS, LANES), F32
                )


def is_level(value):
    axis = value.ndim - 3
    return lax.broadcasted_iota(jnp.int32, value.shape, axis) == value.shape[axis] - 1


def unit_of(value, rows):
    tile = value[..., -1:, :rows, :].astype(F32)
    tile = tile * tile
    tile = tile * tile
    return jnp.broadcast_to(tile * tile, value.shape)


def encode(value, rows):
    return jnp.where(is_level(value), value, value * (32768.0 / unit_of(value, rows))).astype(F16)


def decode(message, rows):
    value = message.astype(F32)
    return jnp.where(is_level(value), value, value * (unit_of(message, rows) * (1.0 / 32768.0)))


def combine(first, second):
    return jnp.where(is_level(first), jnp.maximum(first, second), first + second)


def level_of(bound):
    level = jnp.full(bound.shape, 2.0**-12, F32)
    for k in range(-11, 9):
        level = jnp.where(bound > 2.0 ** (8 * (k - 1)), 2.0**k, level)
    return level


def top(value):
    return jnp.max(jnp.max(jnp.abs(value), axis=1, keepdims=True), axis=0, keepdims=True)


def wgrad_pair(tiles, ref, flip, xst, dref, width):
    turned = xst.T
    for lo, hi in chunks(2 * width):
        if hi <= width:
            upper = dref[:, lo:hi]
            lower = dref[:, width + lo : width + hi]
        elif lo >= width:
            upper = dref[:, lo:hi]
            lower = -dref[:, lo - width : hi - width]
        else:
            upper = dref[:, lo:hi]
            lower = jnp.concatenate([dref[:, width + lo :], -dref[:, : hi - width]], 1)
        tiles.store(ref, flip, mm(turned, jnp.concatenate([upper, lower], 0)), lo)
    tiles.blank(ref, flip)


def hand_out(tiles, full, level, keep, send):
    tail = jnp.broadcast_to(level, (ROWS, LANES))
    for k, out in enumerate((keep, send)):
        for q in range(tiles.parts // 2):

            def step(g, carry):
                out[q, g, : tiles.each] = full[k, q, g, : tiles.each]
                out[q, g, tiles.each] = tail
                return carry

            lax.fori_loop(0, tiles.graph, step, 0)


def make_first(channels, heads, tiles, size, marks):
    z, w1, w2 = LEVELS * channels, (LEVELS - 1) * channels, (LEVELS - 2) * channels
    b1 = z + 2 * w1

    def body(
        me, table, cols, wz,
        x1, d1, x2, d2, gate_out, cot_out, feat_zero, level_out, keep, send, *rest,
    ):
        flags, full = rest[:-1], rest[-1]
        for flag, (axis, bit) in zip(flags, marks):
            value = (me[0 if axis == "dp" else 1] >> bit) & 1
            flag[...] = jnp.full((ROWS, LANES), value, jnp.int32).astype(F32)
        count = cols.shape[0]
        atoms = table.shape[1]
        flip = me[0] & 1
        feat = table.at[0]
        cot = table.at[1]
        feat_zero[...] = feat[:, :z]
        pick = one_hot(cols[:, 4:5], (count, atoms), 1).astype(BF16)
        aim = one_hot(cols[:, 5:6], (count, atoms), 1).astype(BF16)
        scale = 1.0 / (channels // heads) ** 0.5
        logits = mm(feat[:, :z], wz[...])
        gate_node = jax.nn.sigmoid(head_sum(logits, channels, heads) * scale)
        gate = sum(mm(pick, part) for part in pieces(gate_node, 3))
        gate_out[...] = gate
        cot_out[...] = mm(aim, cot[...]).astype(BF16)

        def turn(lo, width, cosine, sine, x, d):
            for j in range(width // channels):
                at = slice(lo + j * channels, lo + (j + 1) * channels)
                bt = slice(lo + width + j * channels, lo + width + (j + 1) * channels)
                p = mm(pick, feat[:, at])
                n = mm(pick, feat[:, bt])
                to = slice(j * channels, (j + 1) * channels)
                x[:count, to] = (cosine * p - sine * n).astype(BF16)
                x[count:, to] = (sine * p + cosine * n).astype(BF16)
                p = cot_out[:, at].astype(F32)
                n = cot_out[:, bt].astype(F32)
                d[:, to] = (gate * (cosine * p - sine * n)).astype(BF16)
                d[:, width + j * channels : width + (j + 1) * channels] = (
                    gate * (sine * p + cosine * n)
                ).astype(BF16)

        turn(z, w1, cols[:, 0:1], cols[:, 1:2], x1, d1)
        turn(b1, w2, cols[:, 2:3], cols[:, 3:4], x2, d2)
        wgrad_pair(tiles, full, flip, x1[...], d1, w1)
        bound = top(feat[...].astype(F32)) * top(cot[...].astype(F32)) * (4.1 * count * size * tiles.graph)
        level = level_of(bound)
        level_out[...] = jnp.broadcast_to(level, level_out.shape)
        hand_out(tiles, full, level, keep, send)

    return body


def make_second(channels, tiles):
    w2 = (LEVELS - 2) * channels

    def body(me, x2, d2, level_in, keep, send, full):
        wgrad_pair(tiles, full, me[0] & 1, x2[...], d2, w2)
        hand_out(tiles, full, level_in[0:1, 0:1], keep, send)

    return body


def make_forward(channels, heads):
    z, w1, w2 = LEVELS * channels, (LEVELS - 1) * channels, (LEVELS - 2) * channels
    b1 = z + 2 * w1

    def body(
        feat, cols, rows, x1, x2, gate_in, cot, wz, wo, wt, sums
    ):
        count = cols.shape[0]
        atoms = feat.shape[0]
        gate = gate_in[...]
        pick = one_hot(cols[:, 4:5], (count, atoms), 1).astype(BF16)
        place = one_hot(rows[4:5, :], (atoms, count), 0)
        scale = 1.0 / (channels // heads) ** 0.5

        dgate = jnp.zeros((count, channels), F32)
        node_zero = mm(feat[:, :z], wz[...])
        wide = jnp.concatenate(pieces(node_zero, 3), 0)
        pick_wide = jnp.concatenate([pick, pick, pick], 1)
        for lo, hi in chunks(z):
            out = mm(pick_wide, wide[:, lo:hi])
            term = cot[:, lo:hi].astype(F32) * out
            for k in range((hi - lo) // channels):
                dgate = dgate + term[:, k * channels : (k + 1) * channels]

        def forward(dgate, lo0, width, cosine, sine, x, w):
            rp = x[:count, :]
            rn = x[count:, :]
            for lo, hi in chunks(width):
                wa = w[:, lo:hi]
                wb = w[:, width + lo : width + hi]
                out_p = mm(rp, wa) - mm(rn, wb)
                out_n = mm(rp, wb) + mm(rn, wa)
                p = cot[:, lo0 + lo : lo0 + hi].astype(F32)
                n = cot[:, lo0 + width + lo : lo0 + width + hi].astype(F32)
                term = (cosine * p - sine * n) * out_p + (sine * p + cosine * n) * out_n
                for k in range((hi - lo) // channels):
                    dgate = dgate + term[:, k * channels : (k + 1) * channels]
            return dgate

        dgate = forward(dgate, z, w1, cols[:, 0:1], cols[:, 1:2], x1, wo)
        dgate = forward(dgate, b1, w2, cols[:, 2:3], cols[:, 3:4], x2, wt)
        dlogit = head_sum(dgate, channels, heads) * gate * (1.0 - gate) * scale
        dz = []
        for j in range(LEVELS):
            block = gate * cot[:, j * channels : (j + 1) * channels].astype(F32)
            if j == 0:
                block = block + dlogit
            dz.append(block.astype(BF16))
        dz = jnp.concatenate(dz, 1)

        node_dz = mm(place.astype(BF16), dz)
        parts = pieces(node_dz, 3)
        sums[0] = feat[...]
        for k in range(3):
            sums[k + 1] = parts[k]

    return body


def make_backward(channels):
    z, w1, w2 = LEVELS * channels, (LEVELS - 1) * channels, (LEVELS - 2) * channels
    b1 = z + 2 * w1

    def body(sums, rows, d1, d2, wz, wo, wt, nodes):
        count = rows.shape[1]
        atoms = sums.shape[1]
        place = one_hot(rows[4:5, :], (atoms, count), 0)
        stack = jnp.concatenate([sums[k] for k in (1, 2, 3)], 0)
        back = mm_t(stack, wz[...])
        nodes[:, :z] = back[:atoms] + back[atoms : 2 * atoms] + back[2 * atoms :]

        def backward(lo0, width, cosine, sine, d, w):
            terms = pieces(place * cosine, 2) + pieces(place * sine, 2)
            spread = mm(jnp.concatenate(terms, 0), d[...])
            by_c = spread[:atoms] + spread[atoms : 2 * atoms]
            by_s = spread[2 * atoms : 3 * atoms] + spread[3 * atoms :]
            t1 = by_c[:, :width] + by_s[:, width:]
            t2 = by_c[:, width:] - by_s[:, :width]
            plus = pieces(jnp.concatenate([t1, t2], 1), 2)
            minus = pieces(jnp.concatenate([t2, -t1], 1), 2)
            back = mm_t(jnp.concatenate(plus + minus, 0), w[...])
            nodes[:, lo0 : lo0 + width] = back[:atoms] + back[atoms : 2 * atoms]
            nodes[:, lo0 + width : lo0 + 2 * width] = (
                back[2 * atoms : 3 * atoms] + back[3 * atoms :]
            )

        backward(z, w1, rows[0:1, :], rows[1:2, :], d1, wo)
        backward(b1, w2, rows[2:3, :], rows[3:4, :], d2, wt)

    return body


def slot_of(me, size):
    bits = size.bit_length() - 1
    return sum(((me >> k) & 1) << (bits - 1 - k) for k in range(bits))


def make_zero(tiles, size):
    def body(me, *refs):
        sums, out, full = refs[:size], refs[size], refs[size + 1]
        left = [ref[0].astype(F32).T.astype(BF16) for ref in sums]
        left = jnp.concatenate([part for part in left for _ in range(3)], 1)
        right = jnp.concatenate([ref[k] for ref in sums for k in (1, 2, 3)], 0)
        for lo, hi in chunks(tiles.cols):
            tiles.store(full, 0, mm(left, right[:, lo:hi]), lo)
        tiles.blank(full, 0)
        rows = size * sums[0].shape[1]
        high = jnp.concatenate([ref[1].astype(F32) for ref in sums], 0)
        feats = jnp.concatenate([ref[0].astype(F32) for ref in sums], 0)
        level = level_of(top(feats) * top(high) * (1.02 * rows * tiles.graph))
        slot = slot_of(me[0], size)
        half = size // 2

        def step(g, carry):
            out[g, : tiles.each] = full[slot // half, slot % half, g, : tiles.each]
            out[g, tiles.each] = jnp.broadcast_to(level, (ROWS, LANES))
            return carry

        lax.fori_loop(0, tiles.graph, step, 0)

    return body


def make_output(layouts, size):
    count = len(layouts)

    def body(me, *refs):
        outs, flats = refs[size * count : size * count + count], refs[size * count + count :]
        for k, tiles in enumerate(layouts):
            parts, out, flat = refs[size * k : size * (k + 1)], outs[k], flats[k]
            for mask in range(size):
                flat[slot_of(me[0] ^ mask, size)] = parts[mask][: tiles.each] * (1.0 / size)
            for tile in range(tiles.count):
                i, j = tile // tiles.across, tile % tiles.across
                r0, r1 = i * ROWS, min((i + 1) * ROWS, tiles.rows)
                out[r0:r1, j * LANES : (j + 1) * LANES] = flat[
                    tile // tiles.each, tile % tiles.each, : r1 - r0
                ]

    return body


def call(body, outs, flops, mib, *args, scratch=(), scalars=1):
    vmem = pl.BlockSpec(memory_space=pltpu.VMEM)
    smem = pl.BlockSpec(memory_space=pltpu.SMEM)
    return pl.pallas_call(
        body,
        out_shape=outs,
        in_specs=[smem] * scalars + [vmem] * (len(args) - scalars),
        out_specs=jax.tree.map(lambda _: vmem, outs),
        scratch_shapes=scratch,
        compiler_params=pltpu.CompilerParams(vmem_limit_bytes=(mib << 20) + sum(ref.get_array_aval().size * 4 for ref in scratch)),
        cost_estimate=pl.CostEstimate(flops=flops, bytes_accessed=1 << 22, transcendentals=0),
    )(*args)


def swap(value, bit, axis="dp"):
    size = lax.axis_size(axis)
    return lax.ppermute(value, axis, [(i, i ^ (1 << bit)) for i in range(size)])


def shards(node_feats, node_cotan, source, target, angle, w_zero, w_one, w_two):
    atom_count = node_feats.shape[1]
    row_width = node_feats.shape[2]
    channels = row_width // 29
    edges = source.shape[1]
    graph = lax.axis_size("graph")
    size = lax.axis_size("dp")
    bits = size.bit_length() - 1
    position = lax.axis_index("graph")
    me = jnp.stack([lax.axis_index("dp"), position])
    reach = atom_count // 2
    atoms = atom_count + 2 * reach
    z, w1, w2 = LEVELS * channels, (LEVELS - 1) * channels, (LEVELS - 2) * channels
    shape = jax.ShapeDtypeStruct

    up = [(i, i + 1) for i in range(graph - 1)]
    down = [(i + 1, i) for i in range(graph - 1)]
    feats, cots = node_feats[0], node_cotan[0]
    before = lax.ppermute(
        jnp.stack([feats[atom_count - reach :], cots[atom_count - reach :]], 0), "graph", up
    )
    after = lax.ppermute(jnp.stack([feats[:reach], cots[:reach]], 0), "graph", down)
    first_atom = position * atom_count - reach
    src = (source[0] - first_atom).astype(F32)
    dst = (target[0] - first_atom).astype(F32)
    phases = angle[0]
    twice = 2.0 * phases
    trig = [jnp.cos(phases), jnp.sin(phases), jnp.cos(twice), jnp.sin(twice)]
    rows = jnp.stack(trig + [src, dst, src, dst], 0)
    cols = rows.T
    table = jnp.concatenate([before, jnp.stack([feats, cots], 0), after], 1)

    t_one = Tiles(*w_one.shape, graph, size)
    t_two = Tiles(*w_two.shape, graph, size)
    t_zero = Tiles(*w_zero.shape, graph, size, spare=1)

    def halves(tiles, parts):
        return (shape((parts,) + tiles.block, F32), shape((parts,) + tiles.block, F32))

    marks = [("dp", k) for k in range(bits)]
    marks += [("graph", k) for k in reversed(range(graph.bit_length() - 1))]
    x1, d1, x2, d2, gate, cot, feat_zero, level, keep_one, send_one, *flags = call(
        make_first(channels, HEADS, t_one, size, marks),
        (
            shape((2 * edges, w1), BF16),
            shape((edges, 2 * w1), BF16),
            shape((2 * edges, w2), BF16),
            shape((edges, 2 * w2), BF16),
            shape((edges, channels), F32),
            shape((edges, row_width), BF16),
            shape((atoms, z), BF16),
            shape((8, LANES), F32),
        )
        + halves(t_one, size // 2)
        + tuple(shape((ROWS, LANES), F32) for _ in marks),
        3_000_000_000,
        14,
        me,
        table,
        cols,
        w_zero[:, :channels],
        scratch=(t_one.scratch(),),
    )

    flags = dict(zip(marks, flags))

    def halving(value, left, steps, rows=ROWS):
        left = list(left)
        value = value.reshape((2,) * len(left) + value.shape[-3:])
        for axis, bit in steps:
            high = flags[axis, bit] > 0.5
            at = left.index((axis, bit))
            left.pop(at)
            low_half = lax.index_in_dim(value, 0, at, False)
            high_half = lax.index_in_dim(value, 1, at, False)
            send = encode(jnp.where(high, low_half, high_half), rows)
            got = swap(send, bit, axis)
            value = combine(jnp.where(high, high_half, low_half), decode(got, rows))
        return value

    def spread(value):
        parts = {0: value}
        for bit in reversed(range(bits)):
            parts.update({m | (1 << bit): swap(v, bit) for m, v in list(parts.items())})
        return [parts[m] for m in range(size)]

    keep_two, send_two = call(
        make_second(channels, t_two),
        halves(t_two, size // 2),
        1_200_000_000,
        6,
        me,
        x2,
        d2,
        level,
        scratch=(t_two.scratch(),),
    )
    one = combine(keep_one, swap(send_one, 0))
    two = combine(keep_two, swap(send_two, 0))
    over_dp = marks[1:bits]
    over_graph = list(reversed(marks[bits:]))
    one = halving(one, marks[1:], over_graph[:-1] + over_dp + over_graph[-1:])
    two = halving(two, marks[1:], over_dp + over_graph, rows=1)

    sums = call(
        make_forward(channels, HEADS),
        shape((4, atoms, z), BF16),
        4_000_000_000,
        8,
        feat_zero,
        cols,
        rows,
        x1,
        x2,
        gate,
        cot,
        w_zero,
        w_one,
        w_two,
        scalars=0,
    )
    nodes = call(
        make_backward(channels),
        shape((atoms, row_width), F32),
        2_000_000_000,
        8,
        sums,
        rows,
        d1,
        d2,
        w_zero,
        w_one,
        w_two,
        scalars=0,
    )

    from_next = lax.ppermute(nodes[:reach], "graph", down)
    from_prev = lax.ppermute(nodes[atom_count + reach :], "graph", up)
    owned = nodes[reach : reach + atom_count]
    owned = owned + jnp.concatenate([from_prev, from_next], 0)
    grad_nodes = owned.astype(BF16)[None]

    parts = {0: sums}
    for bit in reversed(range(bits)):
        parts.update({m | (1 << bit): swap(v, bit) for m, v in list(parts.items())})
    zero = call(
        make_zero(t_zero, size),
        shape(t_zero.block, F32),
        1_000_000_000,
        8,
        me,
        *[parts[m] for m in range(size)],
        scratch=(t_zero.scratch(),),
    )
    zero = halving(zero, marks[bits:], over_graph[1::-1] + over_graph[2:])
    layouts = (t_zero, t_one, t_two)
    parts = spread(zero) + spread(one) + spread(two)
    grads = call(
        make_output(layouts, size),
        tuple(shape((tiles.rows, tiles.cols), F32) for tiles in layouts),
        50_000_000,
        8,
        me,
        *parts,
        scratch=tuple(
            pltpu.VMEM((size, tiles.each, ROWS, LANES), F32) for tiles in layouts
        ),
    )
    return (grad_nodes, *grads)


def solution(mesh):
    return jax.shard_map(
        shards,
        mesh=mesh,
        in_specs=(
            P("dp", "graph", None),
            P("dp", "graph", None),
            P("dp", "graph"),
            P("dp", "graph"),
            P("dp", "graph"),
            P(),
            P(),
            P(),
        ),
        out_specs=(P("dp", "graph", None), P("graph", None), P("graph", None), P("graph", None)),
        check_vma=False,
    )
```

```python
import jax
import jax.numpy as jnp
from jax import lax
from jax.experimental import pallas as pl
from jax.experimental.pallas import tpu as pltpu
from jax.sharding import PartitionSpec as P


HEADS = 8
LEVELS = 7
ROWS = 16
LANES = 128
F32 = jnp.float32
BF16 = jnp.bfloat16
F16 = jnp.float16


def mm(first, second):
    return lax.dot_general(first, second, (((1,), (0,)), ((), ())), preferred_element_type=F32)


def mm_t(first, second):
    return lax.dot_general(first, second, (((1,), (1,)), ((), ())), preferred_element_type=F32)


def pieces(value, count):
    out = []
    rest = value
    for _ in range(count):
        part = rest.astype(BF16)
        out.append(part)
        rest = rest - part.astype(F32)
    return out


def one_hot(index, shape, dim):
    count = lax.broadcasted_iota(jnp.int32, shape, dim).astype(F32)
    return jnp.where(count == index, 1.0, 0.0).astype(F32)


def chunks(width, step=256):
    return [(lo, min(lo + step, width)) for lo in range(0, width, step)]


def head_mask(channels, heads):
    size = channels // heads
    row = lax.broadcasted_iota(jnp.int32, (channels, channels), 0) // size
    col = lax.broadcasted_iota(jnp.int32, (channels, channels), 1) // size
    return jnp.where(row == col, 1.0, 0.0).astype(BF16)


def head_sum(value, channels, heads):
    mask = head_mask(channels, heads)
    total = None
    for part in pieces(value, 3):
        term = mm(part, mask)
        total = term if total is None else total + term
    return total


class Tiles:
    def __init__(self, rows, cols, graph, parts, spare=0):
        self.rows = rows // graph
        self.cols = cols
        self.graph = graph
        self.down = -(-self.rows // ROWS)
        self.across = cols // LANES
        self.count = self.down * self.across
        self.parts = parts
        self.each = -(-self.count // parts) + spare
        self.block = (graph, self.each + 1, ROWS, LANES)

    def scratch(self):
        return pltpu.VMEM((2, self.parts // 2) + self.block, F32)

    def store(self, ref, flip, block, lo):
        half = self.parts // 2
        for g in range(self.graph):
            for i in range(self.down):
                r0 = i * ROWS
                r1 = min(r0 + ROWS, self.rows)
                for j in range(block.shape[1] // LANES):
                    tile = i * self.across + lo // LANES + j
                    q = tile // self.each
                    ref[flip ^ (q // half), q % half, g, tile % self.each, : r1 - r0, :] = block[
                        g * self.rows + r0 : g * self.rows + r1, j * LANES : (j + 1) * LANES
                    ]

    def blank(self, ref, flip):
        half = self.parts // 2
        for tile in range(self.count, self.parts * self.each):
            q = tile // self.each
            for g in range(self.graph):
                ref[flip ^ (q // half), q % half, g, tile % self.each] = jnp.zeros(
                    (ROWS, LANES), F32
                )


def is_level(value):
    axis = value.ndim - 3
    return lax.broadcasted_iota(jnp.int32, value.shape, axis) == value.shape[axis] - 1


def unit_of(value, rows):
    tile = value[..., -1:, :rows, :].astype(F32)
    tile = tile * tile
    tile = tile * tile
    return jnp.broadcast_to(tile * tile, value.shape)


def encode(value, rows):
    return jnp.where(is_level(value), value, value * (32768.0 / unit_of(value, rows))).astype(F16)


def decode(message, rows):
    value = message.astype(F32)
    return jnp.where(is_level(value), value, value * (unit_of(message, rows) * (1.0 / 32768.0)))


def combine(first, second):
    return jnp.where(is_level(first), jnp.maximum(first, second), first + second)


def level_of(bound):
    level = jnp.full(bound.shape, 2.0**-12, F32)
    for k in range(-11, 9):
        level = jnp.where(bound > 2.0 ** (8 * (k - 1)), 2.0**k, level)
    return level


def top(value):
    return jnp.max(jnp.max(jnp.abs(value), axis=1, keepdims=True), axis=0, keepdims=True)


def wgrad_pair(tiles, ref, flip, xst, dref, width):
    turned = xst.T
    for lo, hi in chunks(2 * width):
        if hi <= width:
            upper = dref[:, lo:hi]
            lower = dref[:, width + lo : width + hi]
        elif lo >= width:
            upper = dref[:, lo:hi]
            lower = -dref[:, lo - width : hi - width]
        else:
            upper = dref[:, lo:hi]
            lower = jnp.concatenate([dref[:, width + lo :], -dref[:, : hi - width]], 1)
        tiles.store(ref, flip, mm(turned, jnp.concatenate([upper, lower], 0)), lo)
    tiles.blank(ref, flip)


def hand_out(tiles, full, level, keep, send):
    tail = jnp.broadcast_to(level, (ROWS, LANES))
    for k, out in enumerate((keep, send)):
        for q in range(tiles.parts // 2):

            def step(g, carry):
                out[q, g, : tiles.each] = full[k, q, g, : tiles.each]
                out[q, g, tiles.each] = tail
                return carry

            lax.fori_loop(0, tiles.graph, step, 0)


def make_first(channels, heads, tiles, size, marks):
    z, w1, w2 = LEVELS * channels, (LEVELS - 1) * channels, (LEVELS - 2) * channels
    b1 = z + 2 * w1

    def body(
        me, table, cols, wz,
        x1, d1, x2, d2, gate_out, cot_out, feat_zero, level_out, keep, send, *rest,
    ):
        flags, full = rest[:-1], rest[-1]
        for flag, (axis, bit) in zip(flags, marks):
            value = (me[0 if axis == "dp" else 1] >> bit) & 1
            flag[...] = jnp.full((ROWS, LANES), value, jnp.int32).astype(F32)
        count = cols.shape[0]
        atoms = table.shape[1]
        flip = me[0] & 1
        feat = table.at[0]
        cot = table.at[1]
        feat_zero[...] = feat[:, :z]
        pick = one_hot(cols[:, 4:5], (count, atoms), 1).astype(BF16)
        aim = one_hot(cols[:, 5:6], (count, atoms), 1).astype(BF16)
        scale = 1.0 / (channels // heads) ** 0.5
        logits = mm(feat[:, :z], wz[...])
        gate_node = jax.nn.sigmoid(head_sum(logits, channels, heads) * scale)
        gate = sum(mm(pick, part) for part in pieces(gate_node, 3))
        gate_out[...] = gate
        cot_out[...] = mm(aim, cot[...]).astype(BF16)

        def turn(lo, width, cosine, sine, x, d):
            for j in range(width // channels):
                at = slice(lo + j * channels, lo + (j + 1) * channels)
                bt = slice(lo + width + j * channels, lo + width + (j + 1) * channels)
                p = mm(pick, feat[:, at])
                n = mm(pick, feat[:, bt])
                to = slice(j * channels, (j + 1) * channels)
                x[:count, to] = (cosine * p - sine * n).astype(BF16)
                x[count:, to] = (sine * p + cosine * n).astype(BF16)
                p = cot_out[:, at].astype(F32)
                n = cot_out[:, bt].astype(F32)
                d[:, to] = (gate * (cosine * p - sine * n)).astype(BF16)
                d[:, width + j * channels : width + (j + 1) * channels] = (
                    gate * (sine * p + cosine * n)
                ).astype(BF16)

        turn(z, w1, cols[:, 0:1], cols[:, 1:2], x1, d1)
        turn(b1, w2, cols[:, 2:3], cols[:, 3:4], x2, d2)
        wgrad_pair(tiles, full, flip, x1[...], d1, w1)
        bound = top(feat[...].astype(F32)) * top(cot[...].astype(F32)) * (4.1 * count * size * tiles.graph)
        level = level_of(bound)
        level_out[...] = jnp.broadcast_to(level, level_out.shape)
        hand_out(tiles, full, level, keep, send)

    return body


def make_second(channels, tiles):
    w2 = (LEVELS - 2) * channels

    def body(me, x2, d2, level_in, keep, send, full):
        wgrad_pair(tiles, full, me[0] & 1, x2[...], d2, w2)
        hand_out(tiles, full, level_in[0:1, 0:1], keep, send)

    return body


def make_forward(channels, heads):
    z, w1, w2 = LEVELS * channels, (LEVELS - 1) * channels, (LEVELS - 2) * channels
    b1 = z + 2 * w1

    def body(
        feat, cols, rows, x1, x2, gate_in, cot, wz, wo, wt, sums
    ):
        count = cols.shape[0]
        atoms = feat.shape[0]
        gate = gate_in[...]
        pick = one_hot(cols[:, 4:5], (count, atoms), 1).astype(BF16)
        place = one_hot(rows[4:5, :], (atoms, count), 0)
        scale = 1.0 / (channels // heads) ** 0.5

        dgate = jnp.zeros((count, channels), F32)
        node_zero = mm(feat[:, :z], wz[...])
        wide = jnp.concatenate(pieces(node_zero, 3), 0)
        pick_wide = jnp.concatenate([pick, pick, pick], 1)
        for lo, hi in chunks(z):
            out = mm(pick_wide, wide[:, lo:hi])
            term = cot[:, lo:hi].astype(F32) * out
            for k in range((hi - lo) // channels):
                dgate = dgate + term[:, k * channels : (k + 1) * channels]

        def forward(dgate, lo0, width, cosine, sine, x, w):
            rp = x[:count, :]
            rn = x[count:, :]
            for lo, hi in chunks(width):
                wa = w[:, lo:hi]
                wb = w[:, width + lo : width + hi]
                out_p = mm(rp, wa) - mm(rn, wb)
                out_n = mm(rp, wb) + mm(rn, wa)
                p = cot[:, lo0 + lo : lo0 + hi].astype(F32)
                n = cot[:, lo0 + width + lo : lo0 + width + hi].astype(F32)
                term = (cosine * p - sine * n) * out_p + (sine * p + cosine * n) * out_n
                for k in range((hi - lo) // channels):
                    dgate = dgate + term[:, k * channels : (k + 1) * channels]
            return dgate

        dgate = forward(dgate, z, w1, cols[:, 0:1], cols[:, 1:2], x1, wo)
        dgate = forward(dgate, b1, w2, cols[:, 2:3], cols[:, 3:4], x2, wt)
        dlogit = head_sum(dgate, channels, heads) * gate * (1.0 - gate) * scale
        dz = []
        for j in range(LEVELS):
            block = gate * cot[:, j * channels : (j + 1) * channels].astype(F32)
            if j == 0:
                block = block + dlogit
            dz.append(block.astype(BF16))
        dz = jnp.concatenate(dz, 1)

        node_dz = mm(place.astype(BF16), dz)
        parts = pieces(node_dz, 3)
        sums[0] = feat[...]
        for k in range(3):
            sums[k + 1] = parts[k]

    return body


def make_backward(channels):
    z, w1, w2 = LEVELS * channels, (LEVELS - 1) * channels, (LEVELS - 2) * channels
    b1 = z + 2 * w1

    def body(sums, rows, d1, d2, wz, wo, wt, nodes):
        count = rows.shape[1]
        atoms = sums.shape[1]
        place = one_hot(rows[4:5, :], (atoms, count), 0)
        stack = jnp.concatenate([sums[k] for k in (1, 2, 3)], 0)
        back = mm_t(stack, wz[...])
        nodes[:, :z] = back[:atoms] + back[atoms : 2 * atoms] + back[2 * atoms :]

        def backward(lo0, width, cosine, sine, d, w):
            terms = pieces(place * cosine, 2) + pieces(place * sine, 2)
            spread = mm(jnp.concatenate(terms, 0), d[...])
            by_c = spread[:atoms] + spread[atoms : 2 * atoms]
            by_s = spread[2 * atoms : 3 * atoms] + spread[3 * atoms :]
            t1 = by_c[:, :width] + by_s[:, width:]
            t2 = by_c[:, width:] - by_s[:, :width]
            plus = pieces(jnp.concatenate([t1, t2], 1), 2)
            minus = pieces(jnp.concatenate([t2, -t1], 1), 2)
            back = mm_t(jnp.concatenate(plus + minus, 0), w[...])
            nodes[:, lo0 : lo0 + width] = back[:atoms] + back[atoms : 2 * atoms]
            nodes[:, lo0 + width : lo0 + 2 * width] = (
                back[2 * atoms : 3 * atoms] + back[3 * atoms :]
            )

        backward(z, w1, rows[0:1, :], rows[1:2, :], d1, wo)
        backward(b1, w2, rows[2:3, :], rows[3:4, :], d2, wt)

    return body


def slot_of(me, size):
    bits = size.bit_length() - 1
    return sum(((me >> k) & 1) << (bits - 1 - k) for k in range(bits))


def make_zero(tiles, size):
    def body(me, *refs):
        sums, out, full = refs[:size], refs[size], refs[size + 1]
        left = [ref[0].astype(F32).T.astype(BF16) for ref in sums]
        left = jnp.concatenate([part for part in left for _ in range(3)], 1)
        right = jnp.concatenate([ref[k] for ref in sums for k in (1, 2, 3)], 0)
        for lo, hi in chunks(tiles.cols):
            tiles.store(full, 0, mm(left, right[:, lo:hi]), lo)
        tiles.blank(full, 0)
        rows = size * sums[0].shape[1]
        high = jnp.concatenate([ref[1].astype(F32) for ref in sums], 0)
        feats = jnp.concatenate([ref[0].astype(F32) for ref in sums], 0)
        level = level_of(top(feats) * top(high) * (1.02 * rows * tiles.graph))
        slot = slot_of(me[0], size)
        half = size // 2

        def step(g, carry):
            out[g, : tiles.each] = full[slot // half, slot % half, g, : tiles.each]
            out[g, tiles.each] = jnp.broadcast_to(level, (ROWS, LANES))
            return carry

        lax.fori_loop(0, tiles.graph, step, 0)

    return body


def make_output(layouts, size):
    count = len(layouts)

    def body(me, *refs):
        outs, flats = refs[size * count : size * count + count], refs[size * count + count :]
        for k, tiles in enumerate(layouts):
            parts, out, flat = refs[size * k : size * (k + 1)], outs[k], flats[k]
            for mask in range(size):
                flat[slot_of(me[0] ^ mask, size)] = parts[mask][: tiles.each] * (1.0 / size)
            for tile in range(tiles.count):
                i, j = tile // tiles.across, tile % tiles.across
                r0, r1 = i * ROWS, min((i + 1) * ROWS, tiles.rows)
                out[r0:r1, j * LANES : (j + 1) * LANES] = flat[
                    tile // tiles.each, tile % tiles.each, : r1 - r0
                ]

    return body


def call(body, outs, flops, mib, *args, scratch=(), scalars=1):
    vmem = pl.BlockSpec(memory_space=pltpu.VMEM)
    smem = pl.BlockSpec(memory_space=pltpu.SMEM)
    return pl.pallas_call(
        body,
        out_shape=outs,
        in_specs=[smem] * scalars + [vmem] * (len(args) - scalars),
        out_specs=jax.tree.map(lambda _: vmem, outs),
        scratch_shapes=scratch,
        compiler_params=pltpu.CompilerParams(vmem_limit_bytes=(mib << 20) + sum(ref.get_array_aval().size * 4 for ref in scratch)),
        cost_estimate=pl.CostEstimate(flops=flops, bytes_accessed=1 << 22, transcendentals=0),
    )(*args)


def swap(value, bit, axis="dp"):
    size = lax.axis_size(axis)
    return lax.ppermute(value, axis, [(i, i ^ (1 << bit)) for i in range(size)])


def shards(node_feats, node_cotan, source, target, angle, w_zero, w_one, w_two):
    atom_count = node_feats.shape[1]
    row_width = node_feats.shape[2]
    channels = row_width // 29
    edges = source.shape[1]
    graph = lax.axis_size("graph")
    size = lax.axis_size("dp")
    bits = size.bit_length() - 1
    position = lax.axis_index("graph")
    me = jnp.stack([lax.axis_index("dp"), position])
    reach = atom_count // 2
    atoms = atom_count + 2 * reach
    z, w1, w2 = LEVELS * channels, (LEVELS - 1) * channels, (LEVELS - 2) * channels
    shape = jax.ShapeDtypeStruct

    up = [(i, i + 1) for i in range(graph - 1)]
    down = [(i + 1, i) for i in range(graph - 1)]
    feats, cots = node_feats[0], node_cotan[0]
    before = lax.ppermute(
        jnp.stack([feats[atom_count - reach :], cots[atom_count - reach :]], 0), "graph", up
    )
    after = lax.ppermute(jnp.stack([feats[:reach], cots[:reach]], 0), "graph", down)
    first_atom = position * atom_count - reach
    src = (source[0] - first_atom).astype(F32)
    dst = (target[0] - first_atom).astype(F32)
    phases = angle[0]
    twice = 2.0 * phases
    trig = [jnp.cos(phases), jnp.sin(phases), jnp.cos(twice), jnp.sin(twice)]
    rows = jnp.stack(trig + [src, dst, src, dst], 0)
    cols = rows.T
    table = jnp.concatenate([before, jnp.stack([feats, cots], 0), after], 1)

    t_one = Tiles(*w_one.shape, graph, size)
    t_two = Tiles(*w_two.shape, graph, size)
    t_zero = Tiles(*w_zero.shape, graph, size, spare=1)

    def halves(tiles, parts):
        return (shape((parts,) + tiles.block, F32), shape((parts,) + tiles.block, F32))

    marks = [("dp", k) for k in range(bits)]
    marks += [("graph", k) for k in reversed(range(graph.bit_length() - 1))]
    x1, d1, x2, d2, gate, cot, feat_zero, level, keep_one, send_one, *flags = call(
        make_first(channels, HEADS, t_one, size, marks),
        (
            shape((2 * edges, w1), BF16),
            shape((edges, 2 * w1), BF16),
            shape((2 * edges, w2), BF16),
            shape((edges, 2 * w2), BF16),
            shape((edges, channels), F32),
            shape((edges, row_width), BF16),
            shape((atoms, z), BF16),
            shape((8, LANES), F32),
        )
        + halves(t_one, size // 2)
        + tuple(shape((ROWS, LANES), F32) for _ in marks),
        3_000_000_000,
        14,
        me,
        table,
        cols,
        w_zero[:, :channels],
        scratch=(t_one.scratch(),),
    )

    flags = dict(zip(marks, flags))

    def halving(value, left, steps, rows=ROWS):
        left = list(left)
        value = value.reshape((2,) * len(left) + value.shape[-3:])
        for axis, bit in steps:
            high = flags[axis, bit] > 0.5
            at = left.index((axis, bit))
            left.pop(at)
            low_half = lax.index_in_dim(value, 0, at, False)
            high_half = lax.index_in_dim(value, 1, at, False)
            send = encode(jnp.where(high, low_half, high_half), rows)
            got = swap(send, bit, axis)
            value = combine(jnp.where(high, high_half, low_half), decode(got, rows))
        return value

    def spread(value, rows=ROWS):
        parts = {0: encode(value, rows)}
        for bit in reversed(range(bits)):
            parts.update({m | (1 << bit): swap(v, bit) for m, v in list(parts.items())})
        return [decode(parts[m], rows) for m in range(size)]

    keep_two, send_two = call(
        make_second(channels, t_two),
        halves(t_two, size // 2),
        1_200_000_000,
        6,
        me,
        x2,
        d2,
        level,
        scratch=(t_two.scratch(),),
    )
    one = combine(keep_one, swap(send_one, 0))
    two = combine(keep_two, swap(send_two, 0))
    over_dp = marks[1:bits]
    over_graph = list(reversed(marks[bits:]))
    one = halving(one, marks[1:], over_graph[:-1] + over_dp + over_graph[-1:])
    two = halving(two, marks[1:], over_dp + over_graph, rows=1)

    sums = call(
        make_forward(channels, HEADS),
        shape((4, atoms, z), BF16),
        4_000_000_000,
        8,
        feat_zero,
        cols,
        rows,
        x1,
        x2,
        gate,
        cot,
        w_zero,
        w_one,
        w_two,
        scalars=0,
    )
    nodes = call(
        make_backward(channels),
        shape((atoms, row_width), F32),
        2_000_000_000,
        8,
        sums,
        rows,
        d1,
        d2,
        w_zero,
        w_one,
        w_two,
        scalars=0,
    )

    from_next = lax.ppermute(nodes[:reach], "graph", down)
    from_prev = lax.ppermute(nodes[atom_count + reach :], "graph", up)
    owned = nodes[reach : reach + atom_count]
    owned = owned + jnp.concatenate([from_prev, from_next], 0)
    grad_nodes = owned.astype(BF16)[None]

    parts = {0: sums}
    for bit in reversed(range(bits)):
        parts.update({m | (1 << bit): swap(v, bit) for m, v in list(parts.items())})
    zero = call(
        make_zero(t_zero, size),
        shape(t_zero.block, F32),
        1_000_000_000,
        8,
        me,
        *[parts[m] for m in range(size)],
        scratch=(t_zero.scratch(),),
    )
    zero = halving(zero, marks[bits:], over_graph[1::-1] + over_graph[2:])
    layouts = (t_zero, t_one, t_two)
    parts = spread(zero) + spread(one) + spread(two, rows=1)
    grads = call(
        make_output(layouts, size),
        tuple(shape((tiles.rows, tiles.cols), F32) for tiles in layouts),
        50_000_000,
        8,
        me,
        *parts,
        scratch=tuple(
            pltpu.VMEM((size, tiles.each, ROWS, LANES), F32) for tiles in layouts
        ),
    )
    return (grad_nodes, *grads)


def solution(mesh):
    return jax.shard_map(
        shards,
        mesh=mesh,
        in_specs=(
            P("dp", "graph", None),
            P("dp", "graph", None),
            P("dp", "graph"),
            P("dp", "graph"),
            P("dp", "graph"),
            P(),
            P(),
            P(),
        ),
        out_specs=(P("dp", "graph", None), P("graph", None), P("graph", None), P("graph", None)),
        check_vma=False,
    )
```
